32 devices in a mesh: py: 8 (over y, x, core), px: 4 (over z).
Axes of the slice: x: 2, y: 2, z: 4, core: 2. Of those that a mesh axis runs over, the one named last changes fastest.
Arguments:
- load_terms: float32 [512, 256, 256], P('py', 'px'), may hold values from -6 to 6
- start_values: float32 [512, 256, 256], P('py', 'px'), may hold values from -6 to 6
- reaction_rate: float32 [512, 256, 256], P('py', 'px'), may hold values from 0.1 to 0.9
Outputs:
- corrected: float32 [512, 256, 256], P('py', 'px')
The draws below stay inside these ranges and needn't reach their ends.
All inputs are finite; a program needn't handle non-finite values.
Results may differ from the reference program's by a relative error of at most 0.00002.
Values sent between devices are 32-bit elements; how exact they have to be, the bound alone decides.
A program may use at most 128 MiB of HBM per device.

```python
import jax
import jax.numpy as jnp
from jax import lax

MEMBERS = 256
RATIO = 4
BEFORE = 2
AFTER = 2
INNER = 7
GRID_Y = 512
GRID_X = 256


def shard_levels(stream_key, extent, shards, smallest, high):
    gain = 1.0
    for axis_at, blocks in shards:
        steps = jax.random.uniform(jax.random.fold_in(jax.random.fold_in(stream_key, 6), axis_at), (blocks,), jnp.float32, smallest / len(shards), high / len(shards))
        gain = gain * jnp.repeat(jnp.exp(steps), extent[axis_at] // blocks).reshape((-1,) + (1,) * (len(extent) - 1 - axis_at))
    return gain


def normal_values(stream_key, dims, width, limit, shards=(), kind=jnp.bfloat16):
    gain = shard_levels(stream_key, dims, shards, -0.22, 0.18) if shards else 1.0
    entries = jax.random.normal(stream_key, dims, jnp.float32) * width * gain
    return jnp.minimum(jnp.maximum(entries, -limit), limit).astype(kind)


def setup_inputs(seed: int = 0) -> dict:
    arg_keys = jax.random.split(jax.random.key(seed), 4)
    return {
        "load_terms": normal_values(arg_keys[0], (GRID_Y, GRID_X, MEMBERS), 1.0, 6.0, ((0, 8), (1, 4)), jnp.float32),
        "start_values": normal_values(arg_keys[1], (GRID_Y, GRID_X, MEMBERS), 1.0, 6.0, ((0, 8), (1, 4)), jnp.float32),
        "reaction_rate": jnp.clip(0.1 + 0.79999997 * jax.random.uniform(arg_keys[2], (GRID_Y, GRID_X, MEMBERS), jnp.float32) ** shard_levels(arg_keys[2], (GRID_Y, GRID_X, MEMBERS), ((0, 8), (1, 4)), -0.2, 0.2), 0.1, 0.9),
    }


def around_sum(padded):
    inner_y, inner_x = padded.shape[0] - 2, padded.shape[1] - 2
    middle_rows = lax.slice_in_dim(padded, 1, 1 + inner_y, axis=0)
    middle_columns = lax.slice_in_dim(padded, 1, 1 + inner_x, axis=1)
    return (lax.slice_in_dim(middle_columns, 0, inner_y, axis=0) + lax.slice_in_dim(middle_columns, 2, 2 + inner_y, axis=0)
            + lax.slice_in_dim(middle_rows, 0, inner_x, axis=1) + lax.slice_in_dim(middle_rows, 2, 2 + inner_x, axis=1))


def relax_once(padded, values, load, mass_here):
    return values + 0.8 * (load + around_sum(padded) - (4.0 + mass_here) * values) / (4.0 + mass_here)


def block_means(values):
    cut = values.reshape(values.shape[0] // RATIO, RATIO, values.shape[1] // RATIO, RATIO, values.shape[2])
    return jnp.mean(cut, axis=(1, 3))


def spread_blocks(values):
    return jnp.repeat(jnp.repeat(values, RATIO, axis=0), RATIO, axis=1)


def reference(load_terms, start_values, reaction_rate):
    values = start_values
    for sweep in range(BEFORE):
        values = relax_once(jnp.pad(values, ((1, 1), (1, 1), (0, 0)), mode="wrap"), values, load_terms, reaction_rate)
    defect = load_terms + around_sum(jnp.pad(values, ((1, 1), (1, 1), (0, 0)), mode="wrap")) - (4.0 + reaction_rate) * values
    coarse_load, coarse_mass = block_means(defect) * RATIO, block_means(reaction_rate) * RATIO
    coarse_values = jnp.zeros_like(coarse_load)
    for sweep in range(INNER):
        coarse_values = relax_once(jnp.pad(coarse_values, ((1, 1), (1, 1), (0, 0)), mode="wrap"), coarse_values, coarse_load, coarse_mass)
    values = values + spread_blocks(coarse_values)
    for sweep in range(AFTER):
        values = relax_once(jnp.pad(values, ((1, 1), (1, 1), (0, 0)), mode="wrap"), values, load_terms, reaction_rate)
    corrected = values
    return corrected
```

```python
import functools

import jax
import jax.numpy as jnp
from jax import lax
from jax.experimental import pallas as pl
from jax.experimental.pallas import tpu as pltpu
from jax.sharding import PartitionSpec as P

RATIO = 4
BEFORE = 2
AFTER = 2
INNER = 7
PAD = 8
HU = 2
HL = 1
HC = INNER
LANES = 128
DIAGONALS = ((-1, -1), (-1, 1), (1, -1), (1, 1))


def span(step, halo, size, depth):
    if step == 0:
        return halo, halo, size
    if step < 0:
        return halo, halo + size, depth
    return halo + size - depth, halo - depth, depth


def kernel(
    sizes, load_hbm, start_hbm, mass_hbm, out_hbm,
    u0, u1, u2, ld, ms, wt, cl, cm, cw, cva, cvb,
    pack0, pack1, land0, land1, tmp, spread, in_sem, out_sem, send_sem, recv_sem,
):
    ny, nx, members, n_py, n_px = sizes
    cy, cx = ny // RATIO, nx // RATIO
    wide = nx + 2 * PAD
    cwide = cx + 2 * PAD
    halves = [pl.ds(i, LANES) for i in range(0, members, LANES)]
    iy, ix = lax.axis_index("py"), lax.axis_index("px")

    def device(dy, dx):
        return (lax.rem(iy + dy + n_py, n_py), lax.rem(ix + dx + n_px, n_px))

    middle = pl.ds(PAD, nx)
    loads = [
        pltpu.make_async_copy(start_hbm, u0.at[pl.ds(HU, ny), middle], in_sem.at[0]),
        pltpu.make_async_copy(load_hbm, ld.at[pl.ds(HL, ny), middle], in_sem.at[1]),
        pltpu.make_async_copy(mass_hbm, ms.at[pl.ds(HL, ny), middle], in_sem.at[2]),
    ]
    for copy in loads:
        copy.start()

    barrier = pltpu.get_barrier_semaphore()
    around = ((-1, 0), (1, 0), (0, -1), (0, 1)) + DIAGONALS
    for dy, dx in around:
        pl.semaphore_signal(
            barrier, inc=1, device_id=device(dy, dx), device_id_type=pl.DeviceIdType.MESH
        )
    pl.semaphore_wait(barrier, len(around))

    count = [0]

    def send(src, dst, dy, dx):
        at = count[0]
        count[0] += 1
        copy = pltpu.make_async_remote_copy(
            src_ref=src, dst_ref=dst, send_sem=send_sem.at[at], recv_sem=recv_sem.at[at],
            device_id=device(dy, dx), device_id_type=pl.DeviceIdType.MESH,
        )
        copy.start()
        return copy

    def send_block(ref, dy, dx, halo, rows, columns, depth):
        sy, ty, ly = span(dy, halo, rows, depth)
        sx, tx, lx = span(dx, PAD, columns, PAD)
        return send(
            ref.at[pl.ds(sy, ly), pl.ds(sx, lx)], ref.at[pl.ds(ty, ly), pl.ds(tx, lx)], dy, dx
        )

    def pack_column(buf, side, at, ref, halo, column):
        def group(g, carry):
            for j in range(8):
                buf[side, at, g, j : j + 1, :] = ref[halo + g * 8 + j, column : column + 1, :]
            return carry

        lax.fori_loop(0, ny // 8, group, 0)

    def unpack_column(buf, side, at, ref, halo, column):
        def group(g, carry):
            for j in range(8):
                ref[halo + g * 8 + j, column : column + 1, :] = buf[side, at, g, j : j + 1, :]
            return carry

        lax.fori_loop(0, ny // 8, group, 0)

    first, last = PAD, PAD + nx - 1
    started = []
    loads[0].wait()
    for k in range(2):
        pack_column(pack0, 0, k, u0, HU, first + k)
        pack_column(pack0, 1, k, u0, HU, last - k)
    for dy in (-1, 1):
        started.append(send_block(u0, dy, 0, HU, ny, nx, HU))
    for dy, dx in DIAGONALS:
        started.append(send_block(u0, dy, dx, HU, ny, nx, 1))
    loads[1].wait()
    pack_column(pack0, 0, 2, ld, HL, first)
    pack_column(pack0, 1, 2, ld, HL, last)
    for dy in (-1, 1):
        started.append(send_block(ld, dy, 0, HL, ny, nx, HL))
    loads[2].wait()
    pack_column(pack0, 0, 3, ms, HL, first)
    pack_column(pack0, 1, 3, ms, HL, last)
    for side, dx in ((0, -1), (1, 1)):
        started.append(send(pack0.at[side], land0.at[side], 0, dx))
    for dy in (-1, 1):
        started.append(send_block(ms, dy, 0, HL, ny, nx, HL))

    def coarse_row(rows, half, h, ref, y):
        tmp[h] = rows
        parts = [tmp[h, pl.ds(k, cx, stride=RATIO), :] for k in range(RATIO)]
        ref[HC + y, pl.ds(PAD, cx), half] = (
            (parts[0] + parts[1]) + (parts[2] + parts[3])
        ) * (1.0 / RATIO)

    def mass_row(y, carry):
        for h, half in enumerate(halves):
            rows = [ms[HL + y * RATIO + k, middle, half] for k in range(RATIO)]
            coarse_row((rows[0] + rows[1]) + (rows[2] + rows[3]), half, h, cm, y)
        return carry

    lax.fori_loop(0, cy, mass_row, 0)
    mass_sent = [send_block(cm, dy, dx, HC, cy, cx, HC) for dy, dx in around]

    for copy in started:
        copy.wait_recv()
    for k in range(2):
        unpack_column(land0, 1, k, u0, HU, PAD - 1 - k)
        unpack_column(land0, 0, k, u0, HU, PAD + nx + k)
    for at, ref in ((2, ld), (3, ms)):
        unpack_column(land0, 1, at, ref, HL, PAD - 1)
        unpack_column(land0, 0, at, ref, HL, PAD + nx)

    def weight_row(r, carry):
        for half in halves:
            wt[r, :, half] = 0.8 / (4.0 + ms[r, :, half])
        return carry

    lax.fori_loop(0, ny + 2 * HL, weight_row, 0)

    def neighbours(src, r, half, width):
        here = src[r, :, half]
        total = (
            src[r - 1, :, half] + src[r + 1, :, half]
            + pltpu.roll(here, 1, 0) + pltpu.roll(here, width - 1, 0)
        )
        return here, total

    def sweep_row(src, dst, y, columns=None):
        for half in halves:
            here, total = neighbours(src, HU + y, half, wide)
            new = 0.2 * here + wt[HL + y, :, half] * (ld[HL + y, :, half] + total)
            if columns is None:
                dst[HU + y, :, half] = new
            else:
                dst[HU + y, middle, half] = new[PAD : PAD + nx]

    def sweep(src, dst, begin, end, columns=None):
        def body(y, carry):
            sweep_row(src, dst, y, columns)
            return carry

        lax.fori_loop(begin, end, body, 0)

    sweep(u0, u1, -1, ny + 1)
    sweep(u1, u2, 0, ny, middle)

    for k in range(2):
        pack_column(pack1, 0, k, u2, HU, first + k)
        pack_column(pack1, 1, k, u2, HU, last - k)
    sent1 = [send(pack1.at[side], land1.at[side], 0, dx) for side, dx in ((0, -1), (1, 1))]
    for dy in (-1, 1):
        sent1.append(send_block(u2, dy, 0, HU, ny, nx, HU))
    for dy, dx in DIAGONALS:
        sent1.append(send_block(u2, dy, dx, HU, ny, nx, 1))
    for copy in sent1:
        copy.wait_recv()
    for k in range(2):
        unpack_column(land1, 1, k, u2, HU, PAD - 1 - k)
        unpack_column(land1, 0, k, u2, HU, PAD + nx + k)

    def defect_row(y, carry):
        for h, half in enumerate(halves):
            total = None
            for k in range(RATIO):
                r = y * RATIO + k
                here, beside = neighbours(u2, HU + r, half, wide)
                term = ld[HL + r, :, half] + beside - (4.0 + ms[HL + r, :, half]) * here
                total = term if total is None else total + term
            coarse_row(total[PAD : PAD + nx], half, h, cl, y)
        return carry

    lax.fori_loop(0, cy, defect_row, 0)

    sent2 = [send_block(cl, dy, dx, HC, cy, cx, HC) for dy, dx in around]
    for copy in mass_sent:
        copy.wait_recv()
    crows = cy + 2 * HC

    def coarse_weight(r, carry):
        for half in halves:
            cw[r, :, half] = 0.8 / (4.0 + cm[r, :, half])
        return carry

    lax.fori_loop(0, crows, coarse_weight, 0)
    for copy in sent2:
        copy.wait_recv()

    def coarse_first(r, carry):
        for half in halves:
            cva[r, :, half] = cw[r, :, half] * cl[r, :, half]
        return carry

    lax.fori_loop(0, crows, coarse_first, 0)
    src, dst = cva, cvb
    for step in range(1, INNER):

        def coarse_sweep(r, carry, src=src, dst=dst):
            for half in halves:
                here, total = neighbours(src, r, half, cwide)
                dst[r, :, half] = 0.2 * here + cw[r, :, half] * (cl[r, :, half] + total)
            return carry

        lax.fori_loop(step, crows - step, coarse_sweep, 0)
        src, dst = dst, src
    coarse = src

    begin = PAD - PAD // RATIO
    cells = wide // RATIO

    def correct(cell_row, rows):
        for h, half in enumerate(halves):
            cell = coarse[cell_row, pl.ds(begin, cells), half]
            for k in range(RATIO):
                spread[h, pl.ds(k, cells, stride=RATIO), :] = cell
            whole = spread[h]
            for r in rows:
                u0[r, :, half] = u2[r, :, half] + whole

    def correct_row(y, carry):
        correct(HC + y, [HU + y * RATIO + k for k in range(RATIO)])
        return carry

    for copy in started + mass_sent + sent1 + sent2:
        copy.wait_send()
    correct(HC - 1, list(range(HU)))
    lax.fori_loop(0, cy, correct_row, 0)
    correct(HC + cy, list(range(HU + ny, 2 * HU + ny)))

    sweep(u0, u1, -1, ny + 1)
    chunk = 8
    outs = []
    for c in range(ny // chunk):
        sweep(u1, u2, c * chunk, (c + 1) * chunk, middle)
        copy = pltpu.make_async_copy(
            u2.at[pl.ds(HU + c * chunk, chunk), middle],
            out_hbm.at[pl.ds(c * chunk, chunk)],
            out_sem.at[c],
        )
        copy.start()
        outs.append(copy)
    for copy in outs:
        copy.wait()


def solution(mesh):
    n_py, n_px = mesh.shape["py"], mesh.shape["px"]

    def per_device(load_terms, start_values, reaction_rate):
        ny, nx, members = load_terms.shape
        cy, cx = ny // RATIO, nx // RATIO
        wide, cwide = nx + 2 * PAD, cx + 2 * PAD
        fine = pltpu.VMEM((ny + 2 * HU, wide, members), jnp.float32)
        term = pltpu.VMEM((ny + 2 * HL, wide, members), jnp.float32)
        coarse = pltpu.VMEM((cy + 2 * HC, cwide, members), jnp.float32)
        columns0 = pltpu.VMEM((2, 4, ny // 8, 8, members), jnp.float32)
        columns1 = pltpu.VMEM((2, 2, ny // 8, 8, members), jnp.float32)
        copies = 36
        return pl.pallas_call(
            functools.partial(kernel, (ny, nx, members, n_py, n_px)),
            out_shape=jax.ShapeDtypeStruct(load_terms.shape, jnp.float32),
            in_specs=[pl.BlockSpec(memory_space=pltpu.HBM)] * 3,
            out_specs=pl.BlockSpec(memory_space=pltpu.HBM),
            scratch_shapes=[
                fine, fine, fine, term, term, term,
                coarse, coarse, coarse, coarse, coarse,
                columns0, columns1, columns0, columns1,
                pltpu.VMEM((members // LANES, nx, LANES), jnp.float32),
                pltpu.VMEM((members // LANES, wide, LANES), jnp.float32),
                pltpu.SemaphoreType.DMA((3,)),
                pltpu.SemaphoreType.DMA((ny // 8,)),
                pltpu.SemaphoreType.DMA((copies,)),
                pltpu.SemaphoreType.DMA((copies,)),
            ],
            compiler_params=pltpu.CompilerParams(
                collective_id=0, has_side_effects=True, vmem_limit_bytes=60 * 2**20
            ),
        )(load_terms, start_values, reaction_rate)

    spec = P("py", "px", None)
    return jax.shard_map(
        per_device, mesh=mesh, in_specs=(spec, spec, spec), out_specs=spec, check_vma=False
    )
```

```python
import functools

import jax
import jax.numpy as jnp
from jax import lax
from jax.experimental import pallas as pl
from jax.experimental.pallas import tpu as pltpu
from jax.sharding import PartitionSpec as P

RATIO = 4
BEFORE = 2
AFTER = 2
INNER = 7
PAD = 8
HU = 2
HL = 1
HC = INNER
LANES = 128
DIAGONALS = ((-1, -1), (-1, 1), (1, -1), (1, 1))


def span(step, halo, size, depth):
    if step == 0:
        return halo, halo, size
    if step < 0:
        return halo, halo + size, depth
    return halo + size - depth, halo - depth, depth


def kernel(
    sizes, load_hbm, start_hbm, mass_hbm, out_hbm,
    u0, u1, u2, ld, ms, wt, cl, cm, cw, cva, cvb,
    pack0, pack1, land0, land1, tmp, spread, in_sem, out_sem, send_sem, recv_sem,
):
    ny, nx, members, n_py, n_px = sizes
    cy, cx = ny // RATIO, nx // RATIO
    wide = nx + 2 * PAD
    cwide = cx + 2 * PAD
    halves = [pl.ds(i, LANES) for i in range(0, members, LANES)]
    iy, ix = lax.axis_index("py"), lax.axis_index("px")

    def device(dy, dx):
        return (lax.rem(iy + dy + n_py, n_py), lax.rem(ix + dx + n_px, n_px))

    middle = pl.ds(PAD, nx)
    loads = [
        pltpu.make_async_copy(start_hbm, u0.at[pl.ds(HU, ny), middle], in_sem.at[0]),
        pltpu.make_async_copy(load_hbm, ld.at[pl.ds(HL, ny), middle], in_sem.at[1]),
        pltpu.make_async_copy(mass_hbm, ms.at[pl.ds(HL, ny), middle], in_sem.at[2]),
    ]
    for copy in loads:
        copy.start()

    barrier = pltpu.get_barrier_semaphore()
    around = ((-1, 0), (1, 0), (0, -1), (0, 1)) + DIAGONALS
    for dy, dx in around:
        pl.semaphore_signal(
            barrier, inc=1, device_id=device(dy, dx), device_id_type=pl.DeviceIdType.MESH
        )
    pl.semaphore_wait(barrier, len(around))

    count = [0]

    def send(src, dst, dy, dx):
        at = count[0]
        count[0] += 1
        copy = pltpu.make_async_remote_copy(
            src_ref=src, dst_ref=dst, send_sem=send_sem.at[at], recv_sem=recv_sem.at[at],
            device_id=device(dy, dx), device_id_type=pl.DeviceIdType.MESH,
        )
        copy.start()
        return copy

    def send_block(ref, dy, dx, halo, rows, columns, depth):
        sy, ty, ly = span(dy, halo, rows, depth)
        sx, tx, lx = span(dx, PAD, columns, PAD)
        return send(
            ref.at[pl.ds(sy, ly), pl.ds(sx, lx)], ref.at[pl.ds(ty, ly), pl.ds(tx, lx)], dy, dx
        )

    def pack_column(buf, side, at, ref, halo, column):
        def group(g, carry):
            for j in range(8):
                buf[side, at, g, j : j + 1, :] = ref[halo + g * 8 + j, column : column + 1, :]
            return carry

        lax.fori_loop(0, ny // 8, group, 0)

    def unpack_column(buf, side, at, ref, halo, column):
        def group(g, carry):
            for j in range(8):
                ref[halo + g * 8 + j, column : column + 1, :] = buf[side, at, g, j : j + 1, :]
            return carry

        lax.fori_loop(0, ny // 8, group, 0)

    first, last = PAD, PAD + nx - 1
    started = []
    loads[0].wait()
    for k in range(2):
        pack_column(pack0, 0, k, u0, HU, first + k)
        pack_column(pack0, 1, k, u0, HU, last - k)
    sides = ((0, -1), (1, 1))

    def send_columns(at, length):
        for side, dx in sides:
            piece = pl.ds(at, length)
            started.append(send(pack0.at[side, piece], land0.at[side, piece], 0, dx))

    send_columns(0, 2)
    for dy in (-1, 1):
        started.append(send_block(u0, dy, 0, HU, ny, nx, HU))
    for dy, dx in DIAGONALS:
        started.append(send_block(u0, dy, dx, HU, ny, nx, 1))
    loads[1].wait()
    pack_column(pack0, 0, 2, ld, HL, first)
    pack_column(pack0, 1, 2, ld, HL, last)
    send_columns(2, 1)
    for dy in (-1, 1):
        started.append(send_block(ld, dy, 0, HL, ny, nx, HL))
    loads[2].wait()
    pack_column(pack0, 0, 3, ms, HL, first)
    pack_column(pack0, 1, 3, ms, HL, last)
    send_columns(3, 1)
    for dy in (-1, 1):
        started.append(send_block(ms, dy, 0, HL, ny, nx, HL))

    def coarse_row(rows, half, h, ref, y):
        tmp[h] = rows
        parts = [tmp[h, pl.ds(k, cx, stride=RATIO), :] for k in range(RATIO)]
        ref[HC + y, pl.ds(PAD, cx), half] = (
            (parts[0] + parts[1]) + (parts[2] + parts[3])
        ) * (1.0 / RATIO)

    def mass_row(y, carry):
        for h, half in enumerate(halves):
            rows = [ms[HL + y * RATIO + k, middle, half] for k in range(RATIO)]
            coarse_row((rows[0] + rows[1]) + (rows[2] + rows[3]), half, h, cm, y)
        return carry

    lax.fori_loop(0, cy, mass_row, 0)
    mass_sent = [send_block(cm, dy, dx, HC, cy, cx, HC) for dy, dx in around]

    def weight_inside(r, carry):
        for half in halves:
            wt[r, middle, half] = 0.8 / (4.0 + ms[r, middle, half])
        return carry

    lax.fori_loop(HL, HL + ny, weight_inside, 0)
    for copy in started:
        copy.wait_recv()
    for k in range(2):
        unpack_column(land0, 1, k, u0, HU, PAD - 1 - k)
        unpack_column(land0, 0, k, u0, HU, PAD + nx + k)
    for at, ref in ((2, ld), (3, ms)):
        unpack_column(land0, 1, at, ref, HL, PAD - 1)
        unpack_column(land0, 0, at, ref, HL, PAD + nx)

    def weight_beside(r, carry):
        for half in halves:
            for columns in (pl.ds(0, PAD), pl.ds(PAD + nx, PAD)):
                wt[r, columns, half] = 0.8 / (4.0 + ms[r, columns, half])
        return carry

    lax.fori_loop(HL, HL + ny, weight_beside, 0)
    for r in (0, HL + ny):
        for half in halves:
            wt[r, :, half] = 0.8 / (4.0 + ms[r, :, half])

    def neighbours(src, r, half, width):
        here = src[r, :, half]
        total = (
            src[r - 1, :, half] + src[r + 1, :, half]
            + pltpu.roll(here, 1, 0) + pltpu.roll(here, width - 1, 0)
        )
        return here, total

    def sweep_row(src, dst, y, columns=None):
        for half in halves:
            here, total = neighbours(src, HU + y, half, wide)
            new = 0.2 * here + wt[HL + y, :, half] * (ld[HL + y, :, half] + total)
            if columns is None:
                dst[HU + y, :, half] = new
            else:
                dst[HU + y, middle, half] = new[PAD : PAD + nx]

    def sweep(src, dst, begin, end, columns=None):
        def body(y, carry):
            sweep_row(src, dst, y, columns)
            return carry

        lax.fori_loop(begin, end, body, 0)

    sweep(u0, u1, -1, ny + 1)
    sweep(u1, u2, 0, ny, middle)

    for k in range(2):
        pack_column(pack1, 0, k, u2, HU, first + k)
        pack_column(pack1, 1, k, u2, HU, last - k)
    sent1 = [send(pack1.at[side], land1.at[side], 0, dx) for side, dx in ((0, -1), (1, 1))]
    for dy in (-1, 1):
        sent1.append(send_block(u2, dy, 0, HU, ny, nx, HU))
    for dy, dx in DIAGONALS:
        sent1.append(send_block(u2, dy, dx, HU, ny, nx, 1))
    for copy in sent1:
        copy.wait_recv()
    for k in range(2):
        unpack_column(land1, 1, k, u2, HU, PAD - 1 - k)
        unpack_column(land1, 0, k, u2, HU, PAD + nx + k)

    def defect_row(y, carry):
        for h, half in enumerate(halves):
            total = None
            for k in range(RATIO):
                r = y * RATIO + k
                here, beside = neighbours(u2, HU + r, half, wide)
                term = ld[HL + r, :, half] + beside - (4.0 + ms[HL + r, :, half]) * here
                total = term if total is None else total + term
            coarse_row(total[PAD : PAD + nx], half, h, cl, y)
        return carry

    lax.fori_loop(0, cy, defect_row, 0)

    sent2 = [send_block(cl, dy, dx, HC, cy, cx, HC) for dy, dx in around]
    for copy in mass_sent:
        copy.wait_recv()
    crows = cy + 2 * HC

    def coarse_weight(r, carry):
        for half in halves:
            cw[r, :, half] = 0.8 / (4.0 + cm[r, :, half])
        return carry

    lax.fori_loop(0, crows, coarse_weight, 0)
    for copy in sent2:
        copy.wait_recv()

    def coarse_first(r, carry):
        for half in halves:
            cva[r, :, half] = cw[r, :, half] * cl[r, :, half]
        return carry

    lax.fori_loop(0, crows, coarse_first, 0)
    src, dst = cva, cvb
    for step in range(1, INNER):

        def coarse_sweep(r, carry, src=src, dst=dst):
            for half in halves:
                here, total = neighbours(src, r, half, cwide)
                dst[r, :, half] = 0.2 * here + cw[r, :, half] * (cl[r, :, half] + total)
            return carry

        lax.fori_loop(step, crows - step, coarse_sweep, 0)
        src, dst = dst, src
    coarse = src

    begin = PAD - PAD // RATIO
    cells = wide // RATIO

    def correct(cell_row, rows):
        for h, half in enumerate(halves):
            cell = coarse[cell_row, pl.ds(begin, cells), half]
            for k in range(RATIO):
                spread[h, pl.ds(k, cells, stride=RATIO), :] = cell
            whole = spread[h]
            for r in rows:
                u0[r, :, half] = u2[r, :, half] + whole

    def correct_row(y, carry):
        correct(HC + y, [HU + y * RATIO + k for k in range(RATIO)])
        return carry

    for copy in started + mass_sent + sent1 + sent2:
        copy.wait_send()
    correct(HC - 1, list(range(HU)))
    lax.fori_loop(0, cy, correct_row, 0)
    correct(HC + cy, list(range(HU + ny, 2 * HU + ny)))

    sweep(u0, u1, -1, ny + 1)
    chunk = 8
    outs = []
    for c in range(ny // chunk):
        sweep(u1, u2, c * chunk, (c + 1) * chunk, middle)
        copy = pltpu.make_async_copy(
            u2.at[pl.ds(HU + c * chunk, chunk), middle],
            out_hbm.at[pl.ds(c * chunk, chunk)],
            out_sem.at[c],
        )
        copy.start()
        outs.append(copy)
    for copy in outs:
        copy.wait()


def solution(mesh):
    n_py, n_px = mesh.shape["py"], mesh.shape["px"]

    def per_device(load_terms, start_values, reaction_rate):
        ny, nx, members = load_terms.shape
        cy, cx = ny // RATIO, nx // RATIO
        wide, cwide = nx + 2 * PAD, cx + 2 * PAD
        fine = pltpu.VMEM((ny + 2 * HU, wide, members), jnp.float32)
        term = pltpu.VMEM((ny + 2 * HL, wide, members), jnp.float32)
        coarse = pltpu.VMEM((cy + 2 * HC, cwide, members), jnp.float32)
        columns0 = pltpu.VMEM((2, 4, ny // 8, 8, members), jnp.float32)
        columns1 = pltpu.VMEM((2, 2, ny // 8, 8, members), jnp.float32)
        copies = 40
        return pl.pallas_call(
            functools.partial(kernel, (ny, nx, members, n_py, n_px)),
            out_shape=jax.ShapeDtypeStruct(load_terms.shape, jnp.float32),
            in_specs=[pl.BlockSpec(memory_space=pltpu.HBM)] * 3,
            out_specs=pl.BlockSpec(memory_space=pltpu.HBM),
            scratch_shapes=[
                fine, fine, fine, term, term, term,
                coarse, coarse, coarse, coarse, coarse,
                columns0, columns1, columns0, columns1,
                pltpu.VMEM((members // LANES, nx, LANES), jnp.float32),
                pltpu.VMEM((members // LANES, wide, LANES), jnp.float32),
                pltpu.SemaphoreType.DMA((3,)),
                pltpu.SemaphoreType.DMA((ny // 8,)),
                pltpu.SemaphoreType.DMA((copies,)),
                pltpu.SemaphoreType.DMA((copies,)),
            ],
            compiler_params=pltpu.CompilerParams(
                collective_id=0, has_side_effects=True, vmem_limit_bytes=60 * 2**20
            ),
        )(load_terms, start_values, reaction_rate)

    spec = P("py", "px", None)
    return jax.shard_map(
        per_device, mesh=mesh, in_specs=(spec, spec, spec), out_specs=spec, check_vma=False
    )
```

```python
import functools

import jax
import jax.numpy as jnp
from jax import lax
from jax.experimental import pallas as pl
from jax.experimental.pallas import tpu as pltpu
from jax.sharding import PartitionSpec as P

RATIO = 4
BEFORE = 2
AFTER = 2
INNER = 7
PAD = 8
HU = 2
HL = 1
HC = INNER
LANES = 128
DIAGONALS = ((-1, -1), (-1, 1), (1, -1), (1, 1))


def span(step, halo, size, depth):
    if step == 0:
        return halo, halo, size
    if step < 0:
        return halo, halo + size, depth
    return halo + size - depth, halo - depth, depth


def kernel(
    sizes, load_hbm, start_hbm, mass_hbm, out_hbm,
    u0, u1, u2, ld, ms, wt, cl, cm, cw, cva, cvb,
    pack0, pack1, land0, land1, tmp, spread, in_sem, out_sem, send_sem, recv_sem,
):
    ny, nx, members, n_py, n_px = sizes
    cy, cx = ny // RATIO, nx // RATIO
    wide = nx + 2 * PAD
    cwide = cx + 2 * PAD
    halves = [pl.ds(i, LANES) for i in range(0, members, LANES)]
    iy, ix = lax.axis_index("py"), lax.axis_index("px")

    def device(dy, dx):
        return (lax.rem(iy + dy + n_py, n_py), lax.rem(ix + dx + n_px, n_px))

    middle = pl.ds(PAD, nx)
    loads = [
        pltpu.make_async_copy(start_hbm, u0.at[pl.ds(HU, ny), middle], in_sem.at[0]),
        pltpu.make_async_copy(load_hbm, ld.at[pl.ds(HL, ny), middle], in_sem.at[1]),
        pltpu.make_async_copy(mass_hbm, ms.at[pl.ds(HL, ny), middle], in_sem.at[2]),
    ]
    for copy in loads:
        copy.start()

    barrier = pltpu.get_barrier_semaphore()
    around = ((-1, 0), (1, 0), (0, -1), (0, 1)) + DIAGONALS
    for dy, dx in around:
        pl.semaphore_signal(
            barrier, inc=1, device_id=device(dy, dx), device_id_type=pl.DeviceIdType.MESH
        )
    pl.semaphore_wait(barrier, len(around))

    count = [0]

    def send(src, dst, dy, dx):
        at = count[0]
        count[0] += 1
        copy = pltpu.make_async_remote_copy(
            src_ref=src, dst_ref=dst, send_sem=send_sem.at[at], recv_sem=recv_sem.at[at],
            device_id=device(dy, dx), device_id_type=pl.DeviceIdType.MESH,
        )
        copy.start()
        return copy

    def send_block(ref, dy, dx, halo, rows, columns, depth):
        sy, ty, ly = span(dy, halo, rows, depth)
        sx, tx, lx = span(dx, PAD, columns, PAD)
        return send(
            ref.at[pl.ds(sy, ly), pl.ds(sx, lx)], ref.at[pl.ds(ty, ly), pl.ds(tx, lx)], dy, dx
        )

    def pack_column(buf, side, at, ref, halo, column):
        def group(g, carry):
            for j in range(8):
                buf[side, at, g, j : j + 1, :] = ref[halo + g * 8 + j, column : column + 1, :]
            return carry

        lax.fori_loop(0, ny // 8, group, 0)

    def unpack_column(buf, side, at, ref, halo, column):
        def group(g, carry):
            for j in range(8):
                ref[halo + g * 8 + j, column : column + 1, :] = buf[side, at, g, j : j + 1, :]
            return carry

        lax.fori_loop(0, ny // 8, group, 0)

    first, last = PAD, PAD + nx - 1
    started = []
    loads[0].wait()
    for k in range(2):
        pack_column(pack0, 0, k, u0, HU, first + k)
        pack_column(pack0, 1, k, u0, HU, last - k)
    sides = ((0, -1), (1, 1))

    def send_columns(at, length):
        for side, dx in sides:
            piece = pl.ds(at, length)
            started.append(send(pack0.at[side, piece], land0.at[side, piece], 0, dx))

    send_columns(0, 2)
    for dy in (-1, 1):
        started.append(send_block(u0, dy, 0, HU, ny, nx, HU))
    for dy, dx in DIAGONALS:
        started.append(send_block(u0, dy, dx, HU, ny, nx, 1))
    loads[1].wait()
    pack_column(pack0, 0, 2, ld, HL, first)
    pack_column(pack0, 1, 2, ld, HL, last)
    send_columns(2, 1)
    for dy in (-1, 1):
        started.append(send_block(ld, dy, 0, HL, ny, nx, HL))
    loads[2].wait()
    pack_column(pack0, 0, 3, ms, HL, first)
    pack_column(pack0, 1, 3, ms, HL, last)
    send_columns(3, 1)
    for dy in (-1, 1):
        started.append(send_block(ms, dy, 0, HL, ny, nx, HL))

    def coarse_row(rows, half, h, ref, y):
        tmp[h] = rows
        parts = [tmp[h, pl.ds(k, cx, stride=RATIO), :] for k in range(RATIO)]
        ref[HC + y, pl.ds(PAD, cx), half] = (
            (parts[0] + parts[1]) + (parts[2] + parts[3])
        ) * (1.0 / RATIO)

    def mass_row(y, carry):
        for h, half in enumerate(halves):
            rows = [ms[HL + y * RATIO + k, middle, half] for k in range(RATIO)]
            coarse_row((rows[0] + rows[1]) + (rows[2] + rows[3]), half, h, cm, y)
        return carry

    lax.fori_loop(0, cy, mass_row, 0)
    mass_sent = [send_block(cm, dy, dx, HC, cy, cx, HC) for dy, dx in around]

    def weight_inside(r, carry):
        for half in halves:
            wt[r, middle, half] = 0.8 / (4.0 + ms[r, middle, half])
        return carry

    lax.fori_loop(HL, HL + ny, weight_inside, 0)
    for copy in started:
        copy.wait_recv()
    for k in range(2):
        unpack_column(land0, 1, k, u0, HU, PAD - 1 - k)
        unpack_column(land0, 0, k, u0, HU, PAD + nx + k)
    for at, ref in ((2, ld), (3, ms)):
        unpack_column(land0, 1, at, ref, HL, PAD - 1)
        unpack_column(land0, 0, at, ref, HL, PAD + nx)

    def weight_beside(r, carry):
        for half in halves:
            for columns in (pl.ds(0, PAD), pl.ds(PAD + nx, PAD)):
                wt[r, columns, half] = 0.8 / (4.0 + ms[r, columns, half])
        return carry

    lax.fori_loop(HL, HL + ny, weight_beside, 0)
    for r in (0, HL + ny):
        for half in halves:
            wt[r, :, half] = 0.8 / (4.0 + ms[r, :, half])

    def neighbours(src, r, half, width):
        here = src[r, :, half]
        total = (
            src[r - 1, :, half] + src[r + 1, :, half]
            + pltpu.roll(here, 1, 0) + pltpu.roll(here, width - 1, 0)
        )
        return here, total

    def sweep_row(src, dst, y, columns=None):
        for half in halves:
            here, total = neighbours(src, HU + y, half, wide)
            new = 0.2 * here + wt[HL + y, :, half] * (ld[HL + y, :, half] + total)
            if columns is None:
                dst[HU + y, :, half] = new
            else:
                dst[HU + y, middle, half] = new[PAD : PAD + nx]

    def sweep(src, dst, begin, end, columns=None):
        def body(y, carry):
            sweep_row(src, dst, y, columns)
            return carry

        lax.fori_loop(begin, end, body, 0)

    sweep(u0, u1, -1, ny + 1)
    sweep(u1, u2, 0, HU, middle)
    sweep(u1, u2, ny - HU, ny, middle)
    sent1 = []
    for dy, dx in DIAGONALS:
        sent1.append(send_block(u2, dy, dx, HU, ny, nx, 1))
    for dy in (-1, 1):
        sent1.append(send_block(u2, dy, 0, HU, ny, nx, HU))

    def outer_columns(y, carry):
        for half in halves:
            for begin, at in ((0, PAD), (nx, 0)):
                window = pl.ds(begin, 2 * PAD)
                here = u1[HU + y, window, half]
                total = (
                    u1[HU + y - 1, window, half] + u1[HU + y + 1, window, half]
                    + pltpu.roll(here, 1, 0) + pltpu.roll(here, 2 * PAD - 1, 0)
                )
                new = 0.2 * here + wt[HL + y, window, half] * (ld[HL + y, window, half] + total)
                u2[HU + y, pl.ds(begin + at, PAD), half] = new[at : at + PAD]
        return carry

    lax.fori_loop(HU, ny - HU, outer_columns, 0)
    for k in range(2):
        pack_column(pack1, 0, k, u2, HU, first + k)
        pack_column(pack1, 1, k, u2, HU, last - k)
    sent1 += [send(pack1.at[side], land1.at[side], 0, dx) for side, dx in sides]
    sweep(u1, u2, HU, ny - HU, middle)
    for copy in sent1:
        copy.wait_recv()
    for k in range(2):
        unpack_column(land1, 1, k, u2, HU, PAD - 1 - k)
        unpack_column(land1, 0, k, u2, HU, PAD + nx + k)

    def defect_row(y, carry):
        for h, half in enumerate(halves):
            total = None
            for k in range(RATIO):
                r = y * RATIO + k
                here, beside = neighbours(u2, HU + r, half, wide)
                term = ld[HL + r, :, half] + beside - (4.0 + ms[HL + r, :, half]) * here
                total = term if total is None else total + term
            coarse_row(total[PAD : PAD + nx], half, h, cl, y)
        return carry

    lax.fori_loop(0, cy, defect_row, 0)

    sent2 = [send_block(cl, dy, dx, HC, cy, cx, HC) for dy, dx in around]
    for copy in mass_sent:
        copy.wait_recv()
    crows = cy + 2 * HC

    def coarse_weight(r, carry):
        for half in halves:
            cw[r, :, half] = 0.8 / (4.0 + cm[r, :, half])
        return carry

    lax.fori_loop(0, crows, coarse_weight, 0)
    for copy in sent2:
        copy.wait_recv()

    def coarse_first(r, carry):
        for half in halves:
            cva[r, :, half] = cw[r, :, half] * cl[r, :, half]
        return carry

    lax.fori_loop(0, crows, coarse_first, 0)
    src, dst = cva, cvb
    for step in range(1, INNER):

        def coarse_sweep(r, carry, src=src, dst=dst):
            for half in halves:
                here, total = neighbours(src, r, half, cwide)
                dst[r, :, half] = 0.2 * here + cw[r, :, half] * (cl[r, :, half] + total)
            return carry

        lax.fori_loop(step, crows - step, coarse_sweep, 0)
        src, dst = dst, src
    coarse = src

    begin = PAD - PAD // RATIO
    cells = wide // RATIO

    def correct(cell_row, rows):
        for h, half in enumerate(halves):
            cell = coarse[cell_row, pl.ds(begin, cells), half]
            for k in range(RATIO):
                spread[h, pl.ds(k, cells, stride=RATIO), :] = cell
            whole = spread[h]
            for r in rows:
                u0[r, :, half] = u2[r, :, half] + whole

    def correct_row(y, carry):
        correct(HC + y, [HU + y * RATIO + k for k in range(RATIO)])
        return carry

    for copy in started + mass_sent + sent1 + sent2:
        copy.wait_send()
    correct(HC - 1, list(range(HU)))
    lax.fori_loop(0, cy, correct_row, 0)
    correct(HC + cy, list(range(HU + ny, 2 * HU + ny)))

    sweep(u0, u1, -1, ny + 1)
    chunk = 8
    outs = []
    for c in range(ny // chunk):
        sweep(u1, u2, c * chunk, (c + 1) * chunk, middle)
        copy = pltpu.make_async_copy(
            u2.at[pl.ds(HU + c * chunk, chunk), middle],
            out_hbm.at[pl.ds(c * chunk, chunk)],
            out_sem.at[c],
        )
        copy.start()
        outs.append(copy)
    for copy in outs:
        copy.wait()


def solution(mesh):
    n_py, n_px = mesh.shape["py"], mesh.shape["px"]

    def per_device(load_terms, start_values, reaction_rate):
        ny, nx, members = load_terms.shape
        cy, cx = ny // RATIO, nx // RATIO
        wide, cwide = nx + 2 * PAD, cx + 2 * PAD
        fine = pltpu.VMEM((ny + 2 * HU, wide, members), jnp.float32)
        term = pltpu.VMEM((ny + 2 * HL, wide, members), jnp.float32)
        coarse = pltpu.VMEM((cy + 2 * HC, cwide, members), jnp.float32)
        columns0 = pltpu.VMEM((2, 4, ny // 8, 8, members), jnp.float32)
        columns1 = pltpu.VMEM((2, 2, ny // 8, 8, members), jnp.float32)
        copies = 40
        return pl.pallas_call(
            functools.partial(kernel, (ny, nx, members, n_py, n_px)),
            out_shape=jax.ShapeDtypeStruct(load_terms.shape, jnp.float32),
            in_specs=[pl.BlockSpec(memory_space=pltpu.HBM)] * 3,
            out_specs=pl.BlockSpec(memory_space=pltpu.HBM),
            scratch_shapes=[
                fine, fine, fine, term, term, term,
                coarse, coarse, coarse, coarse, coarse,
                columns0, columns1, columns0, columns1,
                pltpu.VMEM((members // LANES, nx, LANES), jnp.float32),
                pltpu.VMEM((members // LANES, wide, LANES), jnp.float32),
                pltpu.SemaphoreType.DMA((3,)),
                pltpu.SemaphoreType.DMA((ny // 8,)),
                pltpu.SemaphoreType.DMA((copies,)),
                pltpu.SemaphoreType.DMA((copies,)),
            ],
            compiler_params=pltpu.CompilerParams(
                collective_id=0, has_side_effects=True, vmem_limit_bytes=60 * 2**20
            ),
        )(load_terms, start_values, reaction_rate)

    spec = P("py", "px", None)
    return jax.shard_map(
        per_device, mesh=mesh, in_specs=(spec, spec, spec), out_specs=spec, check_vma=False
    )
```
